32 devices in a mesh: dp: 2 (over x), ep: 16 (over y, z, core).
Axes of the slice: x: 2, y: 2, z: 4, core: 2. Of those that a mesh axis runs over, the one named last changes fastest.
Arguments:
- x: bfloat16 [2, 16, 256, 2560], P('dp', 'ep'), parts along dimension 0
- expert: int32 [2, 16, 256, 1], P('dp', 'ep'), parts along dimension 0
- slot: int32 [2, 16, 256, 1], P('dp', 'ep'), parts along dimension 0
- gate: float32 [2, 16, 256, 1], P('dp', 'ep'), parts along dimension 0
- w_gate: bfloat16 [16, 2560, 8192], P('ep')
- w_up: bfloat16 [16, 2560, 8192], P('ep')
- w_down: bfloat16 [16, 8192, 2560], P('ep')
- s_gate: bfloat16 [2560, 8192], replicated
- s_up: bfloat16 [2560, 8192], replicated
- s_down: bfloat16 [8192, 2560], replicated
Outputs:
- y: bfloat16 [2, 16, 256, 2560], P('dp', 'ep'), parts along dimension 0
There are 2 independent parts. The reference program is written for one: setup_inputs(seed, part) draws one part's arguments, and reference() takes and returns one part's arrays. A program takes and returns all parts, laid end to end along the dimension named above; an argument that names none is the same for every part.
All inputs are finite; a program needn't handle non-finite values.
Results may differ from the reference program's by a relative error of at most 0.009.
Values are sent between devices in bfloat16 or wider.
A program may use at most 2 GiB of HBM per device.

```python
import jax
import jax.numpy as jnp

MEMBERS = 16
TOKENS = 256
D = 2560
FF = 8192
TOP = 1
EXPERTS = 16
SHARED_FF = 8192
SLOTS = 5 * TOKENS * TOP // (4 * EXPERTS)


def setup_inputs(seed: int = 0, part: int = 0) -> dict:
    own, k1, k2, k3, k4, k5, k6 = jax.random.split(jax.random.key(seed), 7)
    kx, ke, kl, kg = jax.random.split(jax.random.fold_in(own, part), 4)
    devices = (1, MEMBERS)
    place = jax.random.permutation(kl, jnp.arange(EXPERTS, dtype=jnp.uint32))
    slow = ((EXPERTS + (9 * place) % EXPERTS) << ((9 * place) // EXPERTS)) // EXPERTS
    wait = (jax.random.bits(ke, (*devices, TOKENS, EXPERTS), jnp.uint32) >> 10) * slow
    expert = jnp.argsort(wait, axis=-1)[..., :TOP].astype(jnp.int32)
    chosen = jax.nn.one_hot(expert, EXPERTS, dtype=jnp.int32)
    in_line = jnp.cumsum(chosen.reshape(*devices, TOKENS * TOP, EXPERTS), axis=2) - 1
    slot = jnp.sum(in_line.reshape(chosen.shape) * chosen, axis=-1)

    def one(key, rows, columns):
        return (jax.random.normal(key, (rows, columns), jnp.float32) * rows**-0.5).astype(jnp.bfloat16)

    def weights(key, rows, columns):
        return jax.lax.map(lambda k: one(k, rows, columns), jax.random.split(key, EXPERTS))

    return {
        "x": jax.random.normal(kx, (*devices, TOKENS, D), jnp.float32).astype(jnp.bfloat16),
        "expert": expert,
        "slot": slot,
        "gate": jax.nn.sigmoid(jax.random.normal(kg, expert.shape, jnp.float32)),
        "w_gate": weights(k1, D, FF),
        "w_up": weights(k2, D, FF),
        "w_down": weights(k3, FF, D),
        "s_gate": one(k4, D, SHARED_FF),
        "s_up": one(k5, D, SHARED_FF),
        "s_down": one(k6, SHARED_FF, D),
    }


def einsum(form, a, b):
    return jnp.einsum(form, a.astype(jnp.float32), b.astype(jnp.float32))


def for_all(x, s_gate, s_up, s_down):
    h = jax.nn.silu(einsum("...d,df->...f", x, s_gate)) * einsum("...d,df->...f", x, s_up)
    return einsum("...f,fd->...d", h.astype(jnp.bfloat16), s_down)


def reference(x, expert, slot, gate, w_gate, w_up, w_down, s_gate, s_up, s_down):
    to_expert = jax.nn.one_hot(expert, EXPERTS, dtype=jnp.bfloat16)
    to_slot = jax.nn.one_hot(slot, SLOTS, dtype=jnp.bfloat16)
    weighted = to_expert * gate[..., None].astype(jnp.bfloat16)
    dispatch = einsum("abtke,abtkc->abtec", to_expert, to_slot).astype(jnp.bfloat16)
    combine = einsum("abtke,abtkc->abtec", weighted, to_slot).astype(jnp.bfloat16)
    z = einsum("abtec,abtd->aebcd", dispatch, x).astype(jnp.bfloat16)
    h = jax.nn.silu(einsum("aebcd,edf->aebcf", z, w_gate))
    h = (h * einsum("aebcd,edf->aebcf", z, w_up)).astype(jnp.bfloat16)
    out = einsum("aebcf,efd->aebcd", h, w_down).astype(jnp.bfloat16)
    y = einsum("abtec,aebcd->abtd", combine, out)
    return (y + for_all(x, s_gate, s_up, s_down)).astype(jnp.bfloat16)
```

```python
import functools

import jax
import jax.numpy as jnp
from jax import lax
from jax.experimental import pallas as pl
from jax.experimental.pallas import tpu as pltpu
from jax.sharding import PartitionSpec as P

MESH = pl.DeviceIdType.MESH
CH = 512
RT = 4
FIRST, EXTRA = 16, 4
LANES = 128
BUFS = 8
PLAN = ((6, 5),)


def mm(a, b):
    return jnp.dot(a, b, preferred_element_type=jnp.float32)


def silu(g):
    return g * jax.nn.sigmoid(g)


def at_col(c, width=CH):
    return pl.ds(c * width if isinstance(c, int) else pl.multiple_of(c * width, width), width)


class Schedule:
    def __init__(self, bufs):
        self.bufs, self.stages = bufs, []

    def add(self, count, *steps):
        self.stages.append((count, steps))
        return len(self.stages) - 1

    def finish(self):
        self.tiles, self.first, at = [], {}, 0
        for s, (count, steps) in enumerate(self.stages):
            for turn in range(count):
                for p, step in enumerate(steps):
                    self.first[s, turn, p] = len(self.tiles)
                    for q, (kind, start, per) in enumerate(step):
                        self.tiles.append((kind, start + per * turn, (s, p, q), turn))
        self.reads, issued = {}, min(self.bufs, len(self.tiles))
        for s, (count, steps) in enumerate(self.stages):
            for turn in range(count):
                for p in range(len(steps)):
                    upto = min(self.first[s, turn, p] + self.bufs, len(self.tiles))
                    self.reads[s, turn, p] = list(range(issued, max(issued, upto)))
                    issued = max(issued, upto)
        assert issued == len(self.tiles)

    def groups(self, s, p):
        found = {}
        for turn in range(self.stages[s][0]):
            for m, n in enumerate(self.reads[s, turn, p]):
                kind, index, where, _ = self.tiles[n]
                found.setdefault((where, m), []).append((turn, kind, index, n))
        out = []
        for entries in found.values():
            while entries:
                run = entries[:2]
                if len(run) == 2:
                    d = [run[1][i] - run[0][i] for i in (0, 2, 3)]
                    for e in entries[2:]:
                        if [e[i] - run[-1][i] for i in (0, 2, 3)] != d:
                            break
                        run.append(e)
                    slope = (d[1] // d[0], d[2] // d[0])
                    assert slope[0] * d[0] == d[1] and slope[1] * d[0] == d[2]
                    gap = d[0]
                else:
                    slope, gap = (0, 0), 1
                t0, kind, i0, n0 = run[0]
                out.append((t0, run[-1][0], gap, kind, (i0, slope[0]), (n0, slope[1])))
                entries = entries[len(run):]
        return out


def kernel(
    plan,
    x_hbm, expert_ref, slot_ref, gate_ref, wg, wu, wd, sg, su, sd, y_hbm,
    ring, x_ref, gates, ups, h_ref, z_out, z_in, r_out, r_in, total, gs, us, hs, acc, zk, send_to, take, fold, unfold, y_ref,
    ring_sem, x_sem, y_sem, z_out_sem, z_in_sem, r_out_sem, r_in_sem,
):
    members, tokens = z_out.shape[1], x_ref.shape[0]
    D, F = x_ref.shape[1], h_ref.shape[1]
    chunks, blocks = D // CH, F // CH
    tile_rows = RT * CH
    groups = F // tile_rows
    me, group = lax.axis_index("ep"), lax.axis_index("dp")

    def peer(d):
        at = me
        for i in range(4):
            if d >> i & 1:
                at = at + (1 << i) * (1 - 2 * ((me // (1 << i)) % 2))
        return (group, at)

    def copies(kind, i, slot):
        if kind in ("sg", "su"):
            w = sg if kind == "sg" else su
            return [(w.at[:, at_col(i)], ring.at[slot, pl.ds(0, D)])]
        if kind == "sd":
            rows = at_col(i)
            return [(sd.at[rows, at_col(c)], ring.at[slot, at_col(c)]) for c in range(chunks)]
        if kind in ("wg", "wu"):
            w = wg if kind == "wg" else wu
            k, b = i // groups, i % groups
            return [(w.at[0, at_col(k), at_col(b * RT + j)], ring.at[slot, at_col(j)]) for j in range(RT)]
        c, b = i // groups, i % groups
        return [(wd.at[0, at_col(b, tile_rows), at_col(c)], ring.at[slot, pl.ds(0, tile_rows)])]

    def read(kind, i, slot):
        for src, dst in copies(kind, i, slot):
            pltpu.make_async_copy(src, dst, ring_sem.at[slot]).start()

    def landed(kind, slot):
        rows = D if kind[0] == "s" else tile_rows
        block = ring.at[slot, pl.ds(0, rows)]
        pltpu.make_async_copy(block, block, ring_sem.at[slot]).wait()

    sched = Schedule(BUFS)

    def enter(s, p, turn):
        count, steps = sched.stages[s]
        for t0, t1, gap, kind, (i0, di), (n0, dn) in sched.groups(s, p):
            def go(kind=kind, t0=t0, i0=i0, di=di, n0=n0, dn=dn):
                past = turn - t0
                read(kind, i0 + di * past, (n0 + dn * past) % BUFS)

            if isinstance(turn, int):
                if t0 <= turn <= t1 and (turn - t0) % gap == 0:
                    go()
            elif t0 == 0 and t1 == count - 1 and gap == 1:
                go()
            else:
                here = jnp.logical_and(turn >= t0, turn <= t1)
                if gap > 1:
                    here = jnp.logical_and(here, (turn - t0 + gap * count) % gap == 0)
                pl.when(here)(go)
        per = sum(len(step) for step in steps)
        slots = [(sched.first[s, 0, p] + per * turn + q) % BUFS for q in range(len(steps[p]))]
        for slot, (kind, _, _) in zip(slots, steps[p]):
            landed(kind, slot)
        return slots

    def run(s, body):
        count = sched.stages[s][0]
        if count == 1:
            body(0)
        elif count > 1:
            lax.fori_loop(0, count, lambda t, c: (body(t), c)[1], 0)

    def shared_up(g_slot, u_slot):
        gs[...] = mm(x_ref[...], ring[g_slot, pl.ds(0, D), :])
        us[...] = mm(x_ref[...], ring[u_slot, pl.ds(0, D), :])

    def shared_h():
        hs[...] = (silu(gs[...]) * us[...]).astype(hs.dtype)

    def shared_down(slot):
        for c in range(chunks):
            total[:, at_col(c)] += mm(hs[...], ring[slot, at_col(c), :])

    def pack(z, out, own, c):
        main = members * FIRST
        out[c, :, :, pl.ds(0, CH)] = z[:main].reshape(members, FIRST, CH)
        rest = jnp.concatenate([z[main:, g * LANES:(g + 1) * LANES] for g in range(CH // LANES)], axis=0)
        rest = mm(fold[...], rest).astype(z.dtype).reshape(members, FIRST, LANES)
        out[c, :, :, pl.ds(CH, LANES)] = rest
        own[c, 0, :, pl.ds(0, CH)] = z[:FIRST]
        own[c, 0, :, pl.ds(CH, LANES)] = rest[0]

    def unpack(box, c):
        main, extra = members * FIRST, members * EXTRA
        zk[pl.ds(0, main), :] = box[c, :, :, pl.ds(0, CH)].reshape(main, CH)
        rest = mm(unfold[...], box[c, :, :, pl.ds(CH, LANES)].reshape(main, LANES)).astype(zk.dtype)
        for g in range(CH // LANES):
            zk[pl.ds(main, extra), pl.ds(g * LANES, LANES)] = rest[g * extra:(g + 1) * extra]

    far_first = sorted(range(1, members), key=lambda d: (0 if d & 4 else 1, -bin(d & 10).count("1"), d))

    def send(out, box, out_sem, in_sem, c):
        for d in far_first:
            pltpu.make_async_remote_copy(
                src_ref=out.at[c, d], dst_ref=box.at[c, d], send_sem=out_sem.at[c], recv_sem=in_sem.at[c],
                device_id=peer(d), device_id_type=MESH,
            ).start()

    def all_of(box, sem, c):
        others = box.at[c, pl.ds(1, members - 1)]
        pltpu.make_async_copy(others, others, sem.at[c]).wait()

    def routed_up(g_slot, u_slot, b):
        for j in range(RT):
            cols = pl.ds(pl.multiple_of(b * tile_rows + j * CH, CH), CH)
            gates[:, cols] += mm(zk[...], ring[g_slot, at_col(j), :])
            ups[:, cols] += mm(zk[...], ring[u_slot, at_col(j), :])

    def routed_h(b):
        for j in range(RT):
            cols = pl.ds(b * tile_rows + j * CH if isinstance(b, int) else pl.multiple_of(b * tile_rows + j * CH, CH), CH)
            h_ref[:, cols] = (silu(gates[:, cols]) * ups[:, cols]).astype(h_ref.dtype)

    stages, block, chunk = [], 0, 0
    for n_shared, n_chunks in plan:
        if n_shared and block == 0:
            stages.append(("first", sched.add(1, [("sg", 0, 0), ("su", 0, 0)]), 0))
            block, n_shared = 1, n_shared - 1
        if n_shared:
            step = [("sg", block, 1), ("su", block, 1), ("sd", block - 1, 1)]
            stages.append(("shared", sched.add(n_shared, step), 0))
            block += n_shared
        plain = min(n_chunks, chunks - 1 - chunk)
        if plain > 0:
            i0 = chunk * groups
            stages.append(("up", sched.add(plain * groups, [("wg", i0, 1), ("wu", i0, 1)]), chunk))
            chunk, n_chunks = chunk + plain, n_chunks - plain
        if n_chunks > 0 and chunk == chunks - 1:
            i0 = chunk * groups
            stages.append(("last", sched.add(groups, [("wg", i0, 1), ("wu", i0, 1)]), chunk))
            chunk += 1
    assert chunk == chunks and block > 0
    halves = groups // 2
    down0 = [[("wd", 2 * p, 0), ("wd", 2 * p + 1, 0)] for p in range(halves)]
    stages.append(("down0", sched.add(1, *down0), 0))
    down = [[("wd", groups + 2 * p, groups), ("wd", groups + 2 * p + 1, groups)] for p in range(halves)]
    stages.append(("down", sched.add(chunks - 1, *down), 1))
    if block < blocks:
        step = [("sg", block, 1), ("su", block, 1), ("sd", block - 1, 1)]
        stages.append(("shared", sched.add(blocks - block, step), 0))
    stages.append(("end", sched.add(1, [("sd", blocks - 1, 0)]), 0))
    sched.finish()

    x_copy = pltpu.make_async_copy(x_hbm.at[0, 0], x_ref, x_sem)
    x_copy.start()
    for n in range(min(BUFS, len(sched.tiles))):
        kind, i, _, _ = sched.tiles[n]
        read(kind, i, n % BUFS)
    barrier = pltpu.get_barrier_semaphore()
    for d in range(1, members):
        pl.semaphore_signal(barrier, inc=1, device_id=peer(d), device_id_type=MESH)

    slots = members * (FIRST + EXTRA)
    main = members * FIRST
    toward = jnp.bitwise_xor(expert_ref[...], me)
    s = slot_ref[...]
    place = jnp.where(s < FIRST, toward * FIRST + s, main + toward * EXTRA + (s - FIRST))
    place = jnp.where(s < FIRST + EXTRA, place, -1)
    weight = gate_ref[...].astype(jnp.bfloat16).astype(jnp.float32)
    square = lax.broadcasted_iota(jnp.int32, (tokens, tokens), 0) == lax.broadcasted_iota(jnp.int32, (tokens, tokens), 1)

    def upright(row):
        return jnp.sum(jnp.where(square, row, jnp.zeros_like(row)), axis=1, keepdims=True)

    rows = lax.broadcasted_iota(jnp.int32, (slots, tokens), 0)
    send_to[...] = jnp.where(rows == place, 1.0, 0.0).astype(send_to.dtype)
    columns = lax.broadcasted_iota(jnp.int32, (tokens, slots), 1)
    take[...] = jnp.where(columns == upright(place), upright(weight), 0.0).astype(take.dtype)
    r = lax.broadcasted_iota(jnp.int32, (main, main), 0)
    q = lax.broadcasted_iota(jnp.int32, (main, main), 1)

    def folded(r, q):
        extra = members * EXTRA
        return (r // EXTRA) % (FIRST // EXTRA) * extra + r // FIRST * EXTRA + r % EXTRA == q

    fold[...] = jnp.where(folded(r, q), 1.0, 0.0).astype(fold.dtype)
    unfold[...] = jnp.where(folded(q, r), 1.0, 0.0).astype(unfold.dtype)

    x_copy.wait()

    def dispatch(c, carry):
        z = mm(send_to[...], x_ref[:, at_col(c)]).astype(z_out.dtype)
        pack(z, z_out, z_in, c)
        return carry

    lax.fori_loop(0, chunks, dispatch, 0)
    pl.semaphore_wait(barrier, members - 1)

    def ship(c, carry):
        send(z_out, z_in, z_out_sem, z_in_sem, c)
        return carry

    lax.fori_loop(0, chunks, ship, 0)

    def clear(c, carry):
        gates[:, at_col(c)] = jnp.zeros((slots, CH), jnp.float32)
        ups[:, at_col(c)] = jnp.zeros((slots, CH), jnp.float32)
        return carry

    lax.fori_loop(0, blocks, clear, 0)
    total[...] = jnp.zeros_like(total)

    def chunk_here(k):
        all_of(z_in, z_in_sem, k)
        unpack(z_in, k)

    def down_steps(stage, turn, c, first):
        for p in range(halves):
            a, b = enter(stage, p, turn)
            if first and p == 0:
                routed_h(groups - 1)
            part = mm(h_ref[:, pl.ds(2 * p * tile_rows, tile_rows)], ring[a, pl.ds(0, tile_rows), :])
            part += mm(h_ref[:, pl.ds((2 * p + 1) * tile_rows, tile_rows)], ring[b, pl.ds(0, tile_rows), :])
            if p > 0:
                part += acc[...]
            if p < halves - 1:
                acc[...] = part
        pack(part.astype(r_out.dtype), r_out, r_in, c)
        send(r_out, r_in, r_out_sem, r_in_sem, c)

    for name, stage, at in stages:
        if name == "first":
            def body(turn, stage=stage):
                shared_up(*enter(stage, 0, turn))
        elif name == "shared":
            def body(turn, stage=stage):
                g, u, d = enter(stage, 0, turn)
                shared_h()
                shared_up(g, u)
                shared_down(d)
        elif name == "up":
            def body(turn, stage=stage, at=at):
                @pl.when(turn % groups == 0)
                def _():
                    chunk_here(at + turn // groups)

                g, u = enter(stage, 0, turn)
                routed_up(g, u, turn % groups)
        elif name == "last":
            chunk_here(at)

            def body(turn, stage=stage):
                g, u = enter(stage, 0, turn)
                routed_h(jnp.maximum(turn - 1, 0))
                routed_up(g, u, turn)
        elif name == "down0":
            def body(turn, stage=stage):
                down_steps(stage, turn, 0, True)
        elif name == "down":
            def body(turn, stage=stage):
                down_steps(stage, turn, turn + 1, False)
        else:
            def body(turn, stage=stage):
                (d,) = enter(stage, 0, turn)
                shared_h()
                shared_down(d)
        run(stage, body)

    def combine(c, carry):
        all_of(r_in, r_in_sem, c)
        unpack(r_in, c)
        y_ref[:, at_col(c)] = (mm(take[...], zk[...]) + total[:, at_col(c)]).astype(y_ref.dtype)
        pltpu.make_async_copy(y_ref.at[:, at_col(c)], y_hbm.at[0, 0, :, at_col(c)], y_sem.at[c]).start()
        return carry

    lax.fori_loop(0, chunks, combine, 0)

    def settle(c, carry):
        all_of(z_out, z_out_sem, c)
        all_of(r_out, r_out_sem, c)
        pltpu.make_async_copy(y_ref.at[:, at_col(c)], y_hbm.at[0, 0, :, at_col(c)], y_sem.at[c]).wait()
        return carry

    lax.fori_loop(0, chunks, settle, 0)


def solution(mesh):
    def step(x, expert, slot, gate, w_gate, w_up, w_down, s_gate, s_up, s_down):
        _, _, tokens, D = x.shape
        F = w_gate.shape[2]
        members = mesh.shape["ep"]
        chunks, slots = D // CH, members * (FIRST + EXTRA)
        bf16, f32 = jnp.bfloat16, jnp.float32
        plan = PLAN
        box = pltpu.VMEM((chunks, members, FIRST, CH + LANES), bf16)
        sems = pltpu.SemaphoreType.DMA((chunks,))
        hbm = pl.BlockSpec(memory_space=pl.ANY)
        vmem = pl.BlockSpec(memory_space=pltpu.VMEM)
        return pl.pallas_call(
            functools.partial(kernel, plan),
            out_shape=jax.ShapeDtypeStruct(x.shape, x.dtype),
            in_specs=[hbm] + [vmem] * 3 + [hbm] * 6,
            out_specs=hbm,
            scratch_shapes=[
                pltpu.VMEM((BUFS, max(D, RT * CH), CH), bf16),
                pltpu.VMEM((tokens, D), bf16),
                pltpu.VMEM((slots, F), f32),
                pltpu.VMEM((slots, F), f32),
                pltpu.VMEM((slots, F), bf16),
                box, box, box, box,
                pltpu.VMEM((tokens, D), f32),
                pltpu.VMEM((tokens, CH), f32),
                pltpu.VMEM((tokens, CH), f32),
                pltpu.VMEM((tokens, CH), bf16),
                pltpu.VMEM((slots, CH), f32),
                pltpu.VMEM((slots, CH), bf16),
                pltpu.VMEM((slots, tokens), bf16),
                pltpu.VMEM((tokens, slots), bf16),
                pltpu.VMEM((members * FIRST, members * FIRST), bf16),
                pltpu.VMEM((members * FIRST, members * FIRST), bf16),
                pltpu.VMEM((tokens, D), bf16),
                pltpu.SemaphoreType.DMA((BUFS,)),
                pltpu.SemaphoreType.DMA,
                sems, sems, sems, sems, sems,
            ],
            compiler_params=pltpu.CompilerParams(
                collective_id=0, has_side_effects=True, vmem_limit_bytes=67_043_328
            ),
        )(
            x, expert.reshape(1, tokens), slot.reshape(1, tokens), gate.reshape(1, tokens),
            w_gate, w_up, w_down, s_gate, s_up, s_down,
        )

    tok, exp, rep = P("dp", "ep", None, None), P("ep", None, None), P(None, None)
    return jax.shard_map(
        step, mesh=mesh, in_specs=(tok,) * 4 + (exp,) * 3 + (rep,) * 3, out_specs=tok, check_vma=False,
    )
```

```python
import functools

import jax
import jax.numpy as jnp
from jax import lax
from jax.experimental import pallas as pl
from jax.experimental.pallas import tpu as pltpu
from jax.sharding import PartitionSpec as P

MESH = pl.DeviceIdType.MESH
CH = 512
RT = 4
FIRST, EXTRA = 16, 4
LANES = 128
BUFS = 8
PLAN = ((4, 5),)


def mm(a, b):
    return jnp.dot(a, b, preferred_element_type=jnp.float32)


def silu(g):
    return g * jax.nn.sigmoid(g)


def at_col(c, width=CH):
    return pl.ds(c * width if isinstance(c, int) else pl.multiple_of(c * width, width), width)


class Schedule:
    def __init__(self, bufs):
        self.bufs, self.stages = bufs, []

    def add(self, count, *steps):
        self.stages.append((count, steps))
        return len(self.stages) - 1

    def finish(self):
        self.tiles, self.first, at = [], {}, 0
        for s, (count, steps) in enumerate(self.stages):
            for turn in range(count):
                for p, step in enumerate(steps):
                    self.first[s, turn, p] = len(self.tiles)
                    for q, (kind, start, per) in enumerate(step):
                        self.tiles.append((kind, start + per * turn, (s, p, q), turn))
        self.reads, issued = {}, min(self.bufs, len(self.tiles))
        for s, (count, steps) in enumerate(self.stages):
            for turn in range(count):
                for p in range(len(steps)):
                    upto = min(self.first[s, turn, p] + self.bufs, len(self.tiles))
                    self.reads[s, turn, p] = list(range(issued, max(issued, upto)))
                    issued = max(issued, upto)
        assert issued == len(self.tiles)

    def groups(self, s, p):
        found = {}
        for turn in range(self.stages[s][0]):
            for m, n in enumerate(self.reads[s, turn, p]):
                kind, index, where, _ = self.tiles[n]
                found.setdefault((where, m), []).append((turn, kind, index, n))
        out = []
        for entries in found.values():
            while entries:
                run = entries[:2]
                if len(run) == 2:
                    d = [run[1][i] - run[0][i] for i in (0, 2, 3)]
                    for e in entries[2:]:
                        if [e[i] - run[-1][i] for i in (0, 2, 3)] != d:
                            break
                        run.append(e)
                    slope = (d[1] // d[0], d[2] // d[0])
                    assert slope[0] * d[0] == d[1] and slope[1] * d[0] == d[2]
                    gap = d[0]
                else:
                    slope, gap = (0, 0), 1
                t0, kind, i0, n0 = run[0]
                out.append((t0, run[-1][0], gap, kind, (i0, slope[0]), (n0, slope[1])))
                entries = entries[len(run):]
        return out


def kernel(
    plan,
    x_hbm, expert_ref, slot_ref, gate_ref, wg, wu, wd, sg, su, sd, y_ref,
    ring, x_ref, gates, ups, h_ref, out_box, z_in, r_in, total, gs, us, hs, acc, zk, send_to, take, fold, unfold,
    ring_sem, x_sem, z_out_sem, z_in_sem, r_out_sem, r_in_sem,
):
    members, tokens = z_in.shape[1], x_ref.shape[0]
    D, F = x_ref.shape[1], h_ref.shape[1]
    chunks, blocks = D // CH, F // CH
    tile_rows = RT * CH
    groups = F // tile_rows
    me, group = lax.axis_index("ep"), lax.axis_index("dp")

    def peer(d):
        at = me
        for i in range(4):
            if d >> i & 1:
                at = at + (1 << i) * (1 - 2 * ((me // (1 << i)) % 2))
        return (group, at)

    def copies(kind, i, slot):
        if kind in ("sg", "su"):
            w = sg if kind == "sg" else su
            return [(w.at[:, at_col(i)], ring.at[slot, pl.ds(0, D)])]
        if kind == "sd":
            rows = at_col(i)
            return [(sd.at[rows, at_col(c)], ring.at[slot, at_col(c)]) for c in range(chunks)]
        if kind in ("wg", "wu"):
            w = wg if kind == "wg" else wu
            k, b = i // groups, i % groups
            return [(w.at[0, at_col(k), at_col(b * RT + j)], ring.at[slot, at_col(j)]) for j in range(RT)]
        c, b = i // groups, i % groups
        return [(wd.at[0, at_col(b, tile_rows), at_col(c)], ring.at[slot, pl.ds(0, tile_rows)])]

    def read(kind, i, slot):
        for src, dst in copies(kind, i, slot):
            pltpu.make_async_copy(src, dst, ring_sem.at[slot]).start()

    def landed(kind, slot):
        rows = D if kind[0] == "s" else tile_rows
        block = ring.at[slot, pl.ds(0, rows)]
        pltpu.make_async_copy(block, block, ring_sem.at[slot]).wait()

    sched = Schedule(BUFS)

    def enter(s, p, turn):
        count, steps = sched.stages[s]
        for t0, t1, gap, kind, (i0, di), (n0, dn) in sched.groups(s, p):
            def go(kind=kind, t0=t0, i0=i0, di=di, n0=n0, dn=dn):
                past = turn - t0
                read(kind, i0 + di * past, (n0 + dn * past) % BUFS)

            if isinstance(turn, int):
                if t0 <= turn <= t1 and (turn - t0) % gap == 0:
                    go()
            elif t0 == 0 and t1 == count - 1 and gap == 1:
                go()
            else:
                here = jnp.logical_and(turn >= t0, turn <= t1)
                if gap > 1:
                    here = jnp.logical_and(here, (turn - t0 + gap * count) % gap == 0)
                pl.when(here)(go)
        per = sum(len(step) for step in steps)
        slots = [(sched.first[s, 0, p] + per * turn + q) % BUFS for q in range(len(steps[p]))]
        for slot, (kind, _, _) in zip(slots, steps[p]):
            landed(kind, slot)
        return slots

    def run(s, body):
        count = sched.stages[s][0]
        if count == 1:
            body(0)
        elif count > 1:
            lax.fori_loop(0, count, lambda t, c: (body(t), c)[1], 0)

    def shared_up(g_slot, u_slot):
        gs[...] = mm(x_ref[...], ring[g_slot, pl.ds(0, D), :])
        us[...] = mm(x_ref[...], ring[u_slot, pl.ds(0, D), :])

    def shared_h():
        hs[...] = (silu(gs[...]) * us[...]).astype(hs.dtype)

    def shared_down(slot):
        for c in range(chunks):
            total[:, at_col(c)] += mm(hs[...], ring[slot, at_col(c), :])

    def pack(z, own, first, n):
        main, parts = members * FIRST, CH // LANES
        rest = [
            jnp.concatenate([z[main:, c * CH + g * LANES:c * CH + (g + 1) * LANES] for g in range(parts)], axis=0)
            for c in range(n)
        ]
        rest = mm(fold[...], jnp.concatenate(rest, axis=1) if n > 1 else rest[0]).astype(z.dtype)
        for c in range(n):
            rows = z[:main, c * CH:(c + 1) * CH].reshape(members, FIRST, CH)
            last = rest[:, c * LANES:(c + 1) * LANES].reshape(members, FIRST, LANES)
            out_box[first + c, :, :, pl.ds(0, CH)] = rows
            out_box[first + c, :, :, pl.ds(CH, LANES)] = last
            own[first + c, 0, :, pl.ds(0, CH)] = rows[0]
            own[first + c, 0, :, pl.ds(CH, LANES)] = last[0]

    def unpack(box, c):
        main, extra = members * FIRST, members * EXTRA
        zk[pl.ds(0, main), :] = box[c, :, :, pl.ds(0, CH)].reshape(main, CH)
        rest = mm(unfold[...], box[c, :, :, pl.ds(CH, LANES)].reshape(main, LANES)).astype(zk.dtype)
        for g in range(CH // LANES):
            zk[pl.ds(main, extra), pl.ds(g * LANES, LANES)] = rest[g * extra:(g + 1) * extra]

    far = sorted((d for d in range(1, members) if d & 4), key=lambda d: (-bin(d & 10).count("1"), d))
    near = sorted((d for d in range(1, members) if not d & 4), key=lambda d: (-bin(d & 10).count("1"), d))
    order = [d for i in range(max(len(far), len(near))) for d in far[i:i + 1] + near[i:i + 1]]

    def send(box, out_sem, in_sem, c):
        for d in order:
            pltpu.make_async_remote_copy(
                src_ref=out_box.at[c, d], dst_ref=box.at[c, d], send_sem=out_sem.at[c], recv_sem=in_sem.at[c],
                device_id=peer(d), device_id_type=MESH,
            ).start()

    def all_of(box, sem, c):
        others = box.at[c, pl.ds(1, members - 1)]
        pltpu.make_async_copy(others, others, sem.at[c]).wait()

    def routed_up(g_slot, u_slot, b, begin):
        for j in range(RT):
            cols = pl.ds(pl.multiple_of(b * tile_rows + j * CH, CH), CH)
            for sums, slot in ((gates, g_slot), (ups, u_slot)):
                part = mm(zk[...], ring[slot, at_col(j), :])
                sums[:, cols] = part if begin else sums[:, cols] + part

    def routed_h(b):
        for j in range(RT):
            cols = pl.ds(b * tile_rows + j * CH if isinstance(b, int) else pl.multiple_of(b * tile_rows + j * CH, CH), CH)
            h_ref[:, cols] = (silu(gates[:, cols]) * ups[:, cols]).astype(h_ref.dtype)

    stages, block, chunk = [], 0, 0
    for n_shared, n_chunks in plan:
        if n_shared and block == 0:
            stages.append(("first", sched.add(1, [("sg", 0, 0), ("su", 0, 0)]), 0))
            block, n_shared = 1, n_shared - 1
        if n_shared:
            step = [("sg", block, 1), ("su", block, 1), ("sd", block - 1, 1)]
            stages.append(("shared", sched.add(n_shared, step), 0))
            block += n_shared
        if n_chunks and chunk == 0:
            stages.append(("begin", sched.add(groups, [("wg", 0, 1), ("wu", 0, 1)]), 0))
            chunk, n_chunks = 1, n_chunks - 1
        plain = min(n_chunks, chunks - 1 - chunk)
        if plain > 0:
            i0 = chunk * groups
            stages.append(("up", sched.add(plain * groups, [("wg", i0, 1), ("wu", i0, 1)]), chunk))
            chunk, n_chunks = chunk + plain, n_chunks - plain
        if n_chunks > 0 and chunk == chunks - 1:
            i0 = chunk * groups
            stages.append(("last", sched.add(groups, [("wg", i0, 1), ("wu", i0, 1)]), chunk))
            chunk += 1
    assert chunk == chunks and block > 0
    halves = groups // 2
    down0 = [[("wd", 2 * p, 0), ("wd", 2 * p + 1, 0)] for p in range(halves)]
    stages.append(("down0", sched.add(1, *down0), 0))
    down = [[("wd", groups + 2 * p, groups), ("wd", groups + 2 * p + 1, groups)] for p in range(halves)]
    stages.append(("down", sched.add(chunks - 1, *down), 1))
    if block < blocks:
        step = [("sg", block, 1), ("su", block, 1), ("sd", block - 1, 1)]
        stages.append(("shared", sched.add(blocks - block, step), 0))
    stages.append(("end", sched.add(1, [("sd", blocks - 1, 0)]), 0))
    sched.finish()

    x_copy = pltpu.make_async_copy(x_hbm.at[0, 0], x_ref, x_sem)
    x_copy.start()
    for n in range(min(BUFS, len(sched.tiles))):
        kind, i, _, _ = sched.tiles[n]
        read(kind, i, n % BUFS)
    barrier = pltpu.get_barrier_semaphore()
    for d in range(1, members):
        pl.semaphore_signal(barrier, inc=1, device_id=peer(d), device_id_type=MESH)

    slots = members * (FIRST + EXTRA)
    main = members * FIRST
    toward = jnp.bitwise_xor(expert_ref[...], me)
    s = slot_ref[...]
    place = jnp.where(s < FIRST, toward * FIRST + s, main + toward * EXTRA + (s - FIRST))
    place = jnp.where(s < FIRST + EXTRA, place, -1)
    weight = gate_ref[...].astype(jnp.bfloat16).astype(jnp.float32)
    square = lax.broadcasted_iota(jnp.int32, (tokens, tokens), 0) == lax.broadcasted_iota(jnp.int32, (tokens, tokens), 1)

    def upright(row):
        return jnp.sum(jnp.where(square, row, jnp.zeros_like(row)), axis=1, keepdims=True)

    rows = lax.broadcasted_iota(jnp.int32, (slots, tokens), 0)
    send_to[...] = jnp.where(rows == place, 1.0, 0.0).astype(send_to.dtype)
    columns = lax.broadcasted_iota(jnp.int32, (tokens, slots), 1)
    take[...] = jnp.where(columns == upright(place), upright(weight), 0.0).astype(take.dtype)
    r = lax.broadcasted_iota(jnp.int32, (main, main), 0)
    q = lax.broadcasted_iota(jnp.int32, (main, main), 1)

    def folded(r, q):
        extra = members * EXTRA
        return (r // EXTRA) % (FIRST // EXTRA) * extra + r // FIRST * EXTRA + r % EXTRA == q

    fold[...] = jnp.where(folded(r, q), 1.0, 0.0).astype(fold.dtype)
    unfold[...] = jnp.where(folded(q, r), 1.0, 0.0).astype(unfold.dtype)

    x_copy.wait()

    pack(mm(send_to[...], x_ref[...]).astype(x_ref.dtype), z_in, 0, chunks)
    pl.semaphore_wait(barrier, members - 1)

    def ship(c, carry):
        send(z_in, z_out_sem, z_in_sem, c)
        return carry

    lax.fori_loop(0, chunks, ship, 0)
    total[...] = jnp.zeros_like(total)

    def chunk_here(k):
        all_of(z_in, z_in_sem, k)
        unpack(z_in, k)

    def down_steps(stage, turn, c, first):
        for p in range(halves):
            a, b = enter(stage, p, turn)
            if first and p == 0:
                routed_h(groups - 1)
            part = mm(h_ref[:, pl.ds(2 * p * tile_rows, tile_rows)], ring[a, pl.ds(0, tile_rows), :])
            part += mm(h_ref[:, pl.ds((2 * p + 1) * tile_rows, tile_rows)], ring[b, pl.ds(0, tile_rows), :])
            if p > 0:
                part += acc[...]
            if p < halves - 1:
                acc[...] = part
        pack(part.astype(x_ref.dtype), r_in, c, 1)
        send(r_in, r_out_sem, r_in_sem, c)

    for name, stage, at in stages:
        if name == "first":
            def body(turn, stage=stage):
                shared_up(*enter(stage, 0, turn))
        elif name == "shared":
            def body(turn, stage=stage):
                g, u, d = enter(stage, 0, turn)
                shared_h()
                shared_up(g, u)
                shared_down(d)
        elif name == "begin":
            chunk_here(0)

            def body(turn, stage=stage):
                g, u = enter(stage, 0, turn)
                routed_up(g, u, turn, True)
        elif name == "up":
            def body(turn, stage=stage, at=at):
                @pl.when(turn % groups == 0)
                def _():
                    chunk_here(at + turn // groups)

                g, u = enter(stage, 0, turn)
                routed_up(g, u, turn % groups, False)
        elif name == "last":
            chunk_here(at)

            def body(turn, stage=stage):
                g, u = enter(stage, 0, turn)
                routed_h(jnp.maximum(turn - 1, 0))
                routed_up(g, u, turn, False)
        elif name == "down0":
            for c in range(chunks):
                all_of(out_box, z_out_sem, c)

            def body(turn, stage=stage):
                down_steps(stage, turn, 0, True)
        elif name == "down":
            def body(turn, stage=stage):
                down_steps(stage, turn, turn + 1, False)
        else:
            def body(turn, stage=stage):
                (d,) = enter(stage, 0, turn)
                shared_h()
                shared_down(d)
        run(stage, body)

    def combine(c, carry):
        all_of(r_in, r_in_sem, c)
        unpack(r_in, c)
        y_ref[0, 0, :, at_col(c)] = (mm(take[...], zk[...]) + total[:, at_col(c)]).astype(y_ref.dtype)
        return carry

    lax.fori_loop(0, chunks, combine, 0)

    def settle(c, carry):
        all_of(out_box, r_out_sem, c)
        return carry

    lax.fori_loop(0, chunks, settle, 0)


def solution(mesh):
    def step(x, expert, slot, gate, w_gate, w_up, w_down, s_gate, s_up, s_down):
        _, _, tokens, D = x.shape
        F = w_gate.shape[2]
        members = mesh.shape["ep"]
        chunks, slots = D // CH, members * (FIRST + EXTRA)
        bf16, f32 = jnp.bfloat16, jnp.float32
        plan = PLAN
        box = pltpu.VMEM((chunks, members, FIRST, CH + LANES), bf16)
        sems = pltpu.SemaphoreType.DMA((chunks,))
        hbm = pl.BlockSpec(memory_space=pl.ANY)
        vmem = pl.BlockSpec(memory_space=pltpu.VMEM)
        return pl.pallas_call(
            functools.partial(kernel, plan),
            out_shape=pltpu.VMEM(x.shape, x.dtype),
            in_specs=[hbm] + [vmem] * 3 + [hbm] * 6,
            out_specs=vmem,
            scratch_shapes=[
                pltpu.VMEM((BUFS, max(D, RT * CH), CH), bf16),
                pltpu.VMEM((tokens, D), bf16),
                pltpu.VMEM((slots, F), f32),
                pltpu.VMEM((slots, F), f32),
                pltpu.VMEM((slots, F), bf16),
                box, box, box,
                pltpu.VMEM((tokens, D), f32),
                pltpu.VMEM((tokens, CH), f32),
                pltpu.VMEM((tokens, CH), f32),
                pltpu.VMEM((tokens, CH), bf16),
                pltpu.VMEM((slots, CH), f32),
                pltpu.VMEM((slots, CH), bf16),
                pltpu.VMEM((slots, tokens), bf16),
                pltpu.VMEM((tokens, slots), bf16),
                pltpu.VMEM((members * FIRST, members * FIRST), bf16),
                pltpu.VMEM((members * FIRST, members * FIRST), bf16),
                pltpu.SemaphoreType.DMA((BUFS,)),
                pltpu.SemaphoreType.DMA,
                sems, sems, sems, sems,
            ],
            compiler_params=pltpu.CompilerParams(
                collective_id=0, has_side_effects=True, vmem_limit_bytes=65_536_000
            ),
        )(
            x, expert.reshape(1, tokens), slot.reshape(1, tokens), gate.reshape(1, tokens),
            w_gate, w_up, w_down, s_gate, s_up, s_down,
        )

    tok, exp, rep = P("dp", "ep", None, None), P("ep", None, None), P(None, None)
    return jax.shard_map(
        step, mesh=mesh, in_specs=(tok,) * 4 + (exp,) * 3 + (rep,) * 3, out_specs=tok, check_vma=False,
    )
```

```python
import functools

import jax
import jax.numpy as jnp
from jax import lax
from jax.experimental import pallas as pl
from jax.experimental.pallas import tpu as pltpu
from jax.sharding import PartitionSpec as P

MESH = pl.DeviceIdType.MESH
CH = 512
RT = 4
FIRST, EXTRA = 16, 4
LANES = 128
BUFS = 8
PLAN = ((9, 5),)


def mm(a, b):
    return jnp.dot(a, b, preferred_element_type=jnp.float32)


def silu(g):
    return g * jax.nn.sigmoid(g)


def at_col(c, width=CH):
    return pl.ds(c * width if isinstance(c, int) else pl.multiple_of(c * width, width), width)


class Schedule:
    def __init__(self, bufs):
        self.bufs, self.stages = bufs, []

    def add(self, count, *steps):
        self.stages.append((count, steps))
        return len(self.stages) - 1

    def finish(self):
        self.tiles, self.first, at = [], {}, 0
        for s, (count, steps) in enumerate(self.stages):
            for turn in range(count):
                for p, step in enumerate(steps):
                    self.first[s, turn, p] = len(self.tiles)
                    for q, (kind, start, per) in enumerate(step):
                        self.tiles.append((kind, start + per * turn, (s, p, q), turn))
        self.reads, issued = {}, min(self.bufs, len(self.tiles))
        for s, (count, steps) in enumerate(self.stages):
            for turn in range(count):
                for p in range(len(steps)):
                    upto = min(self.first[s, turn, p] + self.bufs, len(self.tiles))
                    self.reads[s, turn, p] = list(range(issued, max(issued, upto)))
                    issued = max(issued, upto)
        assert issued == len(self.tiles)

    def groups(self, s, p):
        found = {}
        for turn in range(self.stages[s][0]):
            for m, n in enumerate(self.reads[s, turn, p]):
                kind, index, where, _ = self.tiles[n]
                found.setdefault((where, m), []).append((turn, kind, index, n))
        out = []
        for entries in found.values():
            while entries:
                run = entries[:2]
                if len(run) == 2:
                    d = [run[1][i] - run[0][i] for i in (0, 2, 3)]
                    for e in entries[2:]:
                        if [e[i] - run[-1][i] for i in (0, 2, 3)] != d:
                            break
                        run.append(e)
                    slope = (d[1] // d[0], d[2] // d[0])
                    assert slope[0] * d[0] == d[1] and slope[1] * d[0] == d[2]
                    gap = d[0]
                else:
                    slope, gap = (0, 0), 1
                t0, kind, i0, n0 = run[0]
                out.append((t0, run[-1][0], gap, kind, (i0, slope[0]), (n0, slope[1])))
                entries = entries[len(run):]
        return out


def kernel(
    plan,
    x_hbm, expert_ref, slot_ref, gate_ref, wg, wu, wd, sg, su, sd, y_ref,
    ring, x_ref, gates, ups, h_ref, out_box, z_in, r_in, total, gs, us, hs, acc, zk, send_to, take, fold, unfold,
    ring_sem, x_sem, z_out_sem, z_in_sem, r_out_sem, r_in_sem,
):
    members, tokens = z_in.shape[1], x_ref.shape[0]
    D, F = x_ref.shape[1], h_ref.shape[1]
    chunks, blocks = D // CH, F // CH
    tile_rows = RT * CH
    groups = F // tile_rows
    me, group = lax.axis_index("ep"), lax.axis_index("dp")

    def peer(d):
        at = me
        for i in range(4):
            if d >> i & 1:
                at = at + (1 << i) * (1 - 2 * ((me // (1 << i)) % 2))
        return (group, at)

    def copies(kind, i, slot):
        if kind in ("sg", "su"):
            w = sg if kind == "sg" else su
            return [(w.at[:, at_col(i)], ring.at[slot, pl.ds(0, D)])]
        if kind == "sd":
            rows = at_col(i)
            return [(sd.at[rows, at_col(c)], ring.at[slot, at_col(c)]) for c in range(chunks)]
        if kind in ("wg", "wu"):
            w = wg if kind == "wg" else wu
            k, b = i // groups, i % groups
            return [(w.at[0, at_col(k), at_col(b * RT + j)], ring.at[slot, at_col(j)]) for j in range(RT)]
        c, b = i // groups, i % groups
        return [(wd.at[0, at_col(b, tile_rows), at_col(c)], ring.at[slot, pl.ds(0, tile_rows)])]

    def read(kind, i, slot):
        for src, dst in copies(kind, i, slot):
            pltpu.make_async_copy(src, dst, ring_sem.at[slot]).start()

    def landed(kind, slot):
        rows = D if kind[0] == "s" else tile_rows
        block = ring.at[slot, pl.ds(0, rows)]
        pltpu.make_async_copy(block, block, ring_sem.at[slot]).wait()

    sched = Schedule(BUFS)

    def enter(s, p, turn):
        count, steps = sched.stages[s]
        for t0, t1, gap, kind, (i0, di), (n0, dn) in sched.groups(s, p):
            def go(kind=kind, t0=t0, i0=i0, di=di, n0=n0, dn=dn):
                past = turn - t0
                read(kind, i0 + di * past, (n0 + dn * past) % BUFS)

            if isinstance(turn, int):
                if t0 <= turn <= t1 and (turn - t0) % gap == 0:
                    go()
            elif t0 == 0 and t1 == count - 1 and gap == 1:
                go()
            else:
                here = jnp.logical_and(turn >= t0, turn <= t1)
                if gap > 1:
                    here = jnp.logical_and(here, (turn - t0 + gap * count) % gap == 0)
                pl.when(here)(go)
        per = sum(len(step) for step in steps)
        slots = [(sched.first[s, 0, p] + per * turn + q) % BUFS for q in range(len(steps[p]))]
        for slot, (kind, _, _) in zip(slots, steps[p]):
            landed(kind, slot)
        return slots

    def run(s, body):
        count = sched.stages[s][0]
        if count == 1:
            body(0)
        elif count > 1:
            lax.fori_loop(0, count, lambda t, c: (body(t), c)[1], 0)

    def shared_up(g_slot, u_slot):
        gs[...] = mm(x_ref[...], ring[g_slot, pl.ds(0, D), :])
        us[...] = mm(x_ref[...], ring[u_slot, pl.ds(0, D), :])

    def shared_h():
        hs[...] = (silu(gs[...]) * us[...]).astype(hs.dtype)

    def shared_down(slot):
        for c in range(chunks):
            total[:, at_col(c)] += mm(hs[...], ring[slot, at_col(c), :])

    def pack(z, own, first, n):
        main, parts = members * FIRST, CH // LANES
        rest = [
            jnp.concatenate([z[main:, c * CH + g * LANES:c * CH + (g + 1) * LANES] for g in range(parts)], axis=0)
            for c in range(n)
        ]
        rest = mm(fold[...], jnp.concatenate(rest, axis=1) if n > 1 else rest[0]).astype(z.dtype)
        for c in range(n):
            rows = z[:main, c * CH:(c + 1) * CH].reshape(members, FIRST, CH)
            last = rest[:, c * LANES:(c + 1) * LANES].reshape(members, FIRST, LANES)
            out_box[first + c, :, :, pl.ds(0, CH)] = rows
            out_box[first + c, :, :, pl.ds(CH, LANES)] = last
            own[first + c, 0, :, pl.ds(0, CH)] = rows[0]
            own[first + c, 0, :, pl.ds(CH, LANES)] = last[0]

    def unpack(box, c):
        main, extra = members * FIRST, members * EXTRA
        zk[pl.ds(0, main), :] = box[c, :, :, pl.ds(0, CH)].reshape(main, CH)
        rest = mm(unfold[...], box[c, :, :, pl.ds(CH, LANES)].reshape(main, LANES)).astype(zk.dtype)
        for g in range(CH // LANES):
            zk[pl.ds(main, extra), pl.ds(g * LANES, LANES)] = rest[g * extra:(g + 1) * extra]

    far = sorted((d for d in range(1, members) if d & 4), key=lambda d: (-bin(d & 10).count("1"), d))
    near = sorted((d for d in range(1, members) if not d & 4), key=lambda d: (-bin(d & 10).count("1"), d))
    order = far + near

    def send(box, out_sem, in_sem, c):
        for d in order:
            pltpu.make_async_remote_copy(
                src_ref=out_box.at[c, d], dst_ref=box.at[c, d], send_sem=out_sem.at[c], recv_sem=in_sem.at[c],
                device_id=peer(d), device_id_type=MESH,
            ).start()

    def all_of(box, sem, c):
        others = box.at[c, pl.ds(1, members - 1)]
        pltpu.make_async_copy(others, others, sem.at[c]).wait()

    def routed_up(g_slot, u_slot, b, begin):
        for j in range(RT):
            cols = pl.ds(pl.multiple_of(b * tile_rows + j * CH, CH), CH)
            for sums, slot in ((gates, g_slot), (ups, u_slot)):
                part = mm(zk[...], ring[slot, at_col(j), :])
                sums[:, cols] = part if begin else sums[:, cols] + part

    def routed_h(b):
        for j in range(RT):
            cols = pl.ds(b * tile_rows + j * CH if isinstance(b, int) else pl.multiple_of(b * tile_rows + j * CH, CH), CH)
            h_ref[:, cols] = (silu(gates[:, cols]) * ups[:, cols]).astype(h_ref.dtype)

    stages, block, chunk = [], 0, 0
    for n_shared, n_chunks in plan:
        if n_shared and block == 0:
            stages.append(("first", sched.add(1, [("sg", 0, 0), ("su", 0, 0)]), 0))
            block, n_shared = 1, n_shared - 1
        if n_shared:
            step = [("sg", block, 1), ("su", block, 1), ("sd", block - 1, 1)]
            stages.append(("shared", sched.add(n_shared, step), 0))
            block += n_shared
        if n_chunks and chunk == 0:
            stages.append(("begin", sched.add(groups, [("wg", 0, 1), ("wu", 0, 1)]), 0))
            chunk, n_chunks = 1, n_chunks - 1
        plain = min(n_chunks, chunks - 1 - chunk)
        if plain > 0:
            i0 = chunk * groups
            stages.append(("up", sched.add(plain * groups, [("wg", i0, 1), ("wu", i0, 1)]), chunk))
            chunk, n_chunks = chunk + plain, n_chunks - plain
        if n_chunks > 0 and chunk == chunks - 1:
            i0 = chunk * groups
            stages.append(("last", sched.add(groups, [("wg", i0, 1), ("wu", i0, 1)]), chunk))
            chunk += 1
    assert chunk == chunks and block > 0
    halves = groups // 2
    down0 = [[("wd", 2 * p, 0), ("wd", 2 * p + 1, 0)] for p in range(halves)]
    stages.append(("down0", sched.add(1, *down0), 0))
    down = [[("wd", groups + 2 * p, groups), ("wd", groups + 2 * p + 1, groups)] for p in range(halves)]
    stages.append(("down", sched.add(chunks - 1, *down), 1))
    if block < blocks:
        step = [("sg", block, 1), ("su", block, 1), ("sd", block - 1, 1)]
        stages.append(("shared", sched.add(blocks - block, step), 0))
    stages.append(("end", sched.add(1, [("sd", blocks - 1, 0)]), 0))
    sched.finish()

    x_copy = pltpu.make_async_copy(x_hbm.at[0, 0], x_ref, x_sem)
    x_copy.start()
    for n in range(min(BUFS, len(sched.tiles))):
        kind, i, _, _ = sched.tiles[n]
        read(kind, i, n % BUFS)
    barrier = pltpu.get_barrier_semaphore()
    for d in range(1, members):
        pl.semaphore_signal(barrier, inc=1, device_id=peer(d), device_id_type=MESH)

    slots = members * (FIRST + EXTRA)
    main = members * FIRST
    toward = jnp.bitwise_xor(expert_ref[...], me)
    s = slot_ref[...]
    place = jnp.where(s < FIRST, toward * FIRST + s, main + toward * EXTRA + (s - FIRST))
    place = jnp.where(s < FIRST + EXTRA, place, -1)
    weight = gate_ref[...].astype(jnp.bfloat16).astype(jnp.float32)
    square = lax.broadcasted_iota(jnp.int32, (tokens, tokens), 0) == lax.broadcasted_iota(jnp.int32, (tokens, tokens), 1)

    def upright(row):
        return jnp.sum(jnp.where(square, row, jnp.zeros_like(row)), axis=1, keepdims=True)

    rows = lax.broadcasted_iota(jnp.int32, (slots, tokens), 0)
    send_to[...] = jnp.where(rows == place, 1.0, 0.0).astype(send_to.dtype)
    columns = lax.broadcasted_iota(jnp.int32, (tokens, slots), 1)
    take[...] = jnp.where(columns == upright(place), upright(weight), 0.0).astype(take.dtype)
    r = lax.broadcasted_iota(jnp.int32, (main, main), 0)
    q = lax.broadcasted_iota(jnp.int32, (main, main), 1)

    def folded(r, q):
        extra = members * EXTRA
        return (r // EXTRA) % (FIRST // EXTRA) * extra + r // FIRST * EXTRA + r % EXTRA == q

    fold[...] = jnp.where(folded(r, q), 1.0, 0.0).astype(fold.dtype)
    unfold[...] = jnp.where(folded(q, r), 1.0, 0.0).astype(unfold.dtype)

    x_copy.wait()

    pack(mm(send_to[...], x_ref[...]).astype(x_ref.dtype), z_in, 0, chunks)
    pl.semaphore_wait(barrier, members - 1)

    def ship(c, carry):
        send(z_in, z_out_sem, z_in_sem, c)
        return carry

    lax.fori_loop(0, chunks, ship, 0)
    total[...] = jnp.zeros_like(total)

    def chunk_here(k):
        all_of(z_in, z_in_sem, k)
        unpack(z_in, k)

    def down_steps(stage, turn, c, first):
        for p in range(halves):
            a, b = enter(stage, p, turn)
            if first and p == 0:
                routed_h(groups - 1)
            part = mm(h_ref[:, pl.ds(2 * p * tile_rows, tile_rows)], ring[a, pl.ds(0, tile_rows), :])
            part += mm(h_ref[:, pl.ds((2 * p + 1) * tile_rows, tile_rows)], ring[b, pl.ds(0, tile_rows), :])
            if p > 0:
                part += acc[...]
            if p < halves - 1:
                acc[...] = part
        pack(part.astype(x_ref.dtype), r_in, c, 1)
        send(r_in, r_out_sem, r_in_sem, c)

    for name, stage, at in stages:
        if name == "first":
            def body(turn, stage=stage):
                shared_up(*enter(stage, 0, turn))
        elif name == "shared":
            def body(turn, stage=stage):
                g, u, d = enter(stage, 0, turn)
                shared_h()
                shared_up(g, u)
                shared_down(d)
        elif name == "begin":
            chunk_here(0)

            def body(turn, stage=stage):
                g, u = enter(stage, 0, turn)
                routed_up(g, u, turn, True)
        elif name == "up":
            def body(turn, stage=stage, at=at):
                @pl.when(turn % groups == 0)
                def _():
                    chunk_here(at + turn // groups)

                g, u = enter(stage, 0, turn)
                routed_up(g, u, turn % groups, False)
        elif name == "last":
            chunk_here(at)

            def body(turn, stage=stage):
                g, u = enter(stage, 0, turn)
                routed_h(jnp.maximum(turn - 1, 0))
                routed_up(g, u, turn, False)
        elif name == "down0":
            for c in range(chunks):
                all_of(out_box, z_out_sem, c)

            def body(turn, stage=stage):
                down_steps(stage, turn, 0, True)
        elif name == "down":
            def body(turn, stage=stage):
                down_steps(stage, turn, turn + 1, False)
        else:
            def body(turn, stage=stage):
                (d,) = enter(stage, 0, turn)
                shared_h()
                shared_down(d)
        run(stage, body)

    def combine(c, carry):
        all_of(r_in, r_in_sem, c)
        unpack(r_in, c)
        y_ref[0, 0, :, at_col(c)] = (mm(take[...], zk[...]) + total[:, at_col(c)]).astype(y_ref.dtype)
        return carry

    lax.fori_loop(0, chunks, combine, 0)

    def settle(c, carry):
        all_of(out_box, r_out_sem, c)
        return carry

    lax.fori_loop(0, chunks, settle, 0)


def solution(mesh):
    def step(x, expert, slot, gate, w_gate, w_up, w_down, s_gate, s_up, s_down):
        _, _, tokens, D = x.shape
        F = w_gate.shape[2]
        members = mesh.shape["ep"]
        chunks, slots = D // CH, members * (FIRST + EXTRA)
        bf16, f32 = jnp.bfloat16, jnp.float32
        plan = PLAN
        box = pltpu.VMEM((chunks, members, FIRST, CH + LANES), bf16)
        sems = pltpu.SemaphoreType.DMA((chunks,))
        hbm = pl.BlockSpec(memory_space=pl.ANY)
        vmem = pl.BlockSpec(memory_space=pltpu.VMEM)
        return pl.pallas_call(
            functools.partial(kernel, plan),
            out_shape=pltpu.VMEM(x.shape, x.dtype),
            in_specs=[hbm] + [vmem] * 3 + [hbm] * 6,
            out_specs=vmem,
            scratch_shapes=[
                pltpu.VMEM((BUFS, max(D, RT * CH), CH), bf16),
                pltpu.VMEM((tokens, D), bf16),
                pltpu.VMEM((slots, F), f32),
                pltpu.VMEM((slots, F), f32),
                pltpu.VMEM((slots, F), bf16),
                box, box, box,
                pltpu.VMEM((tokens, D), f32),
                pltpu.VMEM((tokens, CH), f32),
                pltpu.VMEM((tokens, CH), f32),
                pltpu.VMEM((tokens, CH), bf16),
                pltpu.VMEM((slots, CH), f32),
                pltpu.VMEM((slots, CH), bf16),
                pltpu.VMEM((slots, tokens), bf16),
                pltpu.VMEM((tokens, slots), bf16),
                pltpu.VMEM((members * FIRST, members * FIRST), bf16),
                pltpu.VMEM((members * FIRST, members * FIRST), bf16),
                pltpu.SemaphoreType.DMA((BUFS,)),
                pltpu.SemaphoreType.DMA,
                sems, sems, sems, sems,
            ],
            compiler_params=pltpu.CompilerParams(
                collective_id=0, has_side_effects=True, vmem_limit_bytes=65_536_000
            ),
        )(
            x, expert.reshape(1, tokens), slot.reshape(1, tokens), gate.reshape(1, tokens),
            w_gate, w_up, w_down, s_gate, s_up, s_down,
        )

    tok, exp, rep = P("dp", "ep", None, None), P("ep", None, None), P(None, None)
    return jax.shard_map(
        step, mesh=mesh, in_specs=(tok,) * 4 + (exp,) * 3 + (rep,) * 3, out_specs=tok, check_vma=False,
    )
```
